256 devices in a mesh: chan: 64 (over y, z, core), slot: 4 (over x).
Axes of the slice: x: 4, y: 4, z: 8, core: 2. Of those that a mesh axis runs over, the one named last changes fastest.
Arguments:
- visibility: float32 [2, 2, 256, 4, 3844], P(None, None, 'chan', 'slot'), parts along dimension 3, may hold values from -6 to 6
- coherency: bfloat16 [2, 2, 16, 256, 4, 3844], P(None, None, None, 'chan', 'slot'), parts along dimension 4, may hold values from -2 to 2
- jones_start: float32 [2, 2, 64, 256, 62], P(None, None, 'slot', 'chan'), parts along dimension 2, may hold values from -4 to 4
- duals_start: float32 [2, 2, 64, 256, 62], P(None, None, 'slot', 'chan'), parts along dimension 2, may hold values from -2 to 2
Outputs:
- jones_final: float32 [2, 2, 64, 256, 62], P(None, None, 'slot', 'chan'), parts along dimension 2
- consensus: float32 [2, 2, 64, 256, 62], P(None, None, 'slot', 'chan'), parts along dimension 2
- duals_final: float32 [2, 2, 64, 256, 62], P(None, None, 'slot', 'chan'), parts along dimension 2
- norms: float32 [8, 2], P('slot'), parts along dimension 0
The draws below stay inside these ranges and needn't reach their ends.
There are 4 independent parts, one for each index of `slot`. The reference program is written for one: setup_inputs(seed, part) draws one part's arguments, and reference() takes and returns one part's arrays. A program takes and returns all parts, laid end to end along the dimension named above; each array names one. Nothing has to cross between parts.
All inputs are finite; a program needn't handle non-finite values.
Results may differ from the reference program's by a relative error of at most 0.0003.
Values sent between devices are 32-bit elements; how exact they have to be, the bound alone decides.
A program may use at most 128 MiB of HBM per device.

```python
import jax
import jax.numpy as jnp
from jax import lax

STATIONS = 62
DIRS = 16
POLS = 2
TIMES = 1
ITERS = 2
CH_DEV = 4
CHANNELS = 256
PAIRS = 3844
N_CHAN = 64


def block_levels(key, extent, cuts, low, high):
    def one(dim, shards_of):
        heights = jax.random.uniform(jax.random.fold_in(jax.random.fold_in(key, 6), dim), (shards_of,), jnp.float32, low / len(cuts), high / len(cuts))
        return jnp.repeat(jnp.exp(heights), extent[dim] // shards_of).reshape((-1,) + (1,) * (len(extent) - dim - 1))

    level = one(*cuts[0])
    for cut in cuts[1:]:
        level = level * one(*cut)
    return level


def scatter_about(rng, dims, scale, bound, split=(), kind=jnp.bfloat16):
    values = jax.random.normal(rng, dims, jnp.float32) * scale
    if len(split) > 0:
        values = block_levels(rng, dims, split, -0.22, 0.18) * values
    return jnp.clip(values, min=-bound, max=bound).astype(kind)


def setup_inputs(seed: int = 0, part: int = 0) -> dict:
    key_list = jax.random.split(jax.random.key(seed), 5)
    part_splits = jax.random.split(jax.random.fold_in(key_list[4], part), 5)
    visibility = scatter_about(part_splits[0], (2, POLS, CHANNELS, TIMES, PAIRS), 1.0, 6.0, ((2, 64),), jnp.float32)
    coherency = scatter_about(part_splits[1], (2, POLS, DIRS, CHANNELS, TIMES, PAIRS), 0.25, 2.0, ((3, 64),))
    jones_start = scatter_about(part_splits[2], (2, POLS, DIRS, CHANNELS, STATIONS), 0.7, 4.0, ((3, 64),), jnp.float32)
    duals_start = scatter_about(part_splits[3], (2, POLS, DIRS, CHANNELS, STATIONS), 0.3, 2.0, ((3, 64),), jnp.float32)
    return {"visibility": visibility, "coherency": coherency, "jones_start": jones_start, "duals_start": duals_start}


penalty = 8.0
kernel_taps = (0.04, 0.06, 0.1, 0.15, 0.3, 0.15, 0.1, 0.06, 0.04)


def jones_update(visibility, coherency, jones_now, target):
    width = jones_now.shape[-1]
    grid_shape = coherency.shape[1:5] + (width, width)
    sky_real = coherency[0].astype(jnp.float32).reshape(grid_shape)
    sky_imag = coherency[1].astype(jnp.float32).reshape(grid_shape)
    vis_shape = visibility.shape[1:4] + (width, width)
    data_real = visibility[0].reshape(vis_shape)[:, None]
    data_imag = visibility[1].reshape(vis_shape)[:, None]
    left_real = jones_now[0][:, :, :, None, :, None]
    left_imag = jones_now[1][:, :, :, None, :, None]
    right_real = jones_now[0][:, :, :, None, None, :]
    right_imag = jones_now[1][:, :, :, None, None, :]
    crossed = 1.0 - jnp.eye(width, dtype=jnp.float32)
    half_real = left_real * sky_real - left_imag * sky_imag
    half_imag = left_real * sky_imag + left_imag * sky_real
    model_real = half_real * right_real + half_imag * right_imag
    model_imag = half_imag * right_real - half_real * right_imag
    rest_real = (data_real - jnp.sum(model_real, axis=1, keepdims=True) + model_real) * crossed
    rest_imag = (data_imag - jnp.sum(model_imag, axis=1, keepdims=True) + model_imag) * crossed
    weight_real = sky_real * right_real + sky_imag * right_imag
    weight_imag = sky_real * right_imag - sky_imag * right_real
    upper_real = jnp.sum(rest_real * weight_real - rest_imag * weight_imag, axis=(3, 5))
    upper_imag = jnp.sum(rest_real * weight_imag + rest_imag * weight_real, axis=(3, 5))
    lower = jnp.sum(crossed * (sky_real * sky_real + sky_imag * sky_imag) * (right_real * right_real + right_imag * right_imag), axis=(3, 5)) + penalty
    return jnp.stack([(upper_real + penalty * target[0]) / lower, (upper_imag + penalty * target[1]) / lower])


def blocked_update(visibility, coherency, jones_now, target):
    vis_shape = visibility.shape
    vis_blocks = jnp.moveaxis(visibility.reshape(vis_shape[:2] + (N_CHAN, CH_DEV) + vis_shape[3:]), 2, 0)
    coh_shape = coherency.shape
    coh_blocks = jnp.moveaxis(coherency.reshape(coh_shape[:3] + (N_CHAN, CH_DEV) + coh_shape[4:]), 3, 0)
    gain_shape = jones_now.shape
    gain_blocks = jnp.moveaxis(jones_now.reshape(gain_shape[:3] + (N_CHAN, CH_DEV) + gain_shape[4:]), 3, 0)
    target_blocks = jnp.moveaxis(target.reshape(gain_shape[:3] + (N_CHAN, CH_DEV) + gain_shape[4:]), 3, 0)
    updated = lax.map(lambda blocks_in: jones_update(*blocks_in), (vis_blocks, coh_blocks, gain_blocks, target_blocks))
    return jnp.moveaxis(updated, 0, 3).reshape(gain_shape)


def smooth(padded, channels):
    total = kernel_taps[0] * padded[:, :, :, 0:channels]
    for offset in range(1, 9):
        total = total + kernel_taps[offset] * padded[:, :, :, offset:offset + channels]
    return total


def reference(visibility, coherency, jones_start, duals_start):
    channels = jones_start.shape[3]
    entries = jones_start.size
    jones_now = jones_start
    consensus = jones_start
    duals_now = duals_start
    partials = []
    for iteration in range(ITERS):
        jones_now = blocked_update(visibility, coherency, jones_now, consensus - duals_now)
        summed = jones_now + duals_now
        padded = jnp.pad(summed, ((0, 0), (0, 0), (0, 0), (4, 4), (0, 0)))
        fresh = smooth(padded, channels)
        duals_now = duals_now + jones_now - fresh
        primal_gap = jones_now - fresh
        moved = fresh - consensus
        primal = jnp.sum(primal_gap * primal_gap) / entries
        change = penalty * penalty * jnp.sum(moved * moved) / entries
        partials.append(jnp.stack([primal, change]))
        consensus = fresh
    return jones_now, consensus, duals_now, jnp.stack(partials)
```

```python
import functools

import jax
import jax.numpy as jnp
from jax import lax
from jax.experimental import pallas as pl
from jax.experimental.pallas import tpu as pltpu
from jax.sharding import PartitionSpec as P

STATIONS = 62
SIDE = 64
CHANS = 4
PAIRS = STATIONS * STATIONS
LANES = 128
FULL = PAIRS // LANES
TILES = FULL + 1
FLAT = STATIONS * SIDE + 2 * SIDE
BLOCK = 4
BLOCKS = SIDE // BLOCK
ROWS = BLOCK * SIDE

penalty = 8.0
kernel_taps = (0.04, 0.06, 0.1, 0.15, 0.3, 0.15, 0.1, 0.06, 0.04)
F32 = jnp.float32
BF16 = jnp.bfloat16


def to_chan(index):
    return {"chan": index}


def shifted(x, by):
    return x if by == 0 else pltpu.roll(x, (-by) % LANES, axis=1)


def smooth_own(own, channel):
    total = None
    for o in range(-3, 4):
        weight = jnp.where((channel + o >= 0) & (channel + o < CHANS), kernel_taps[o + 4], 0.0)
        term = shifted(own, o) * weight
        total = term if total is None else total + term
    return total


def smooth_sides(low, high, channel):
    total = None
    for o in range(1, 5):
        weight = jnp.where(channel - o < 0, kernel_taps[4 - o], 0.0)
        term = shifted(low, CHANS - o) * weight
        total = term if total is None else total + term
        weight = jnp.where(channel + o >= CHANS, kernel_taps[4 + o], 0.0)
        total = total + shifted(high, o - CHANS) * weight
    return total


def body(
    vis, coh, vis_tail, coh_tail, jones, duals,
    jones_out, cons_out, duals_out, norms_out,
    cbuf, vbuf, ct_re, ct_im, v_re, v_im, h_re, h_im, d_re, d_im, mix,
    g, y, part, sent, from_low, from_high, mine, gather_a, gather_b,
    load_sems, vis_sem, send_low, send_high, low_sem, high_sem,
    a_send, a_recv, b_send, b_recv,
    *, entries,
):
    count = lax.axis_size("chan")
    me = lax.axis_index("chan")
    core = lax.rem(me, 2)
    at_z = lax.rem(me // 2, 8)
    at_y = me // 16
    slot_a = at_y * 2 + core
    slot_b = at_z

    def peer_a(i):
        other = lax.rem(slot_a + i, 8)
        return (other // 2) * 16 + at_z * 2 + lax.rem(other, 2)

    def peer_b(i):
        other = lax.rem(slot_b + i, 8)
        return at_y * 16 + other * 2 + core

    loads = [
        pltpu.make_async_copy(
            coh.at[:, :, pl.ds(LANES * j, LANES)], cbuf.at[j], load_sems.at[j])
        for j in range(FULL)
    ]
    vis_load = pltpu.make_async_copy(
        vis.at[:, 0, pl.ds(0, LANES * FULL)], vbuf, vis_sem)
    for copy in loads:
        copy.start()
    vis_load.start()

    @pl.when(me == 0)
    def _():
        from_low[...] = jnp.zeros_like(from_low)

    @pl.when(me == count - 1)
    def _():
        from_high[...] = jnp.zeros_like(from_high)

    barrier = pltpu.get_barrier_semaphore()
    for i in range(1, 8):
        pl.semaphore_signal(barrier, inc=1, device_id=to_chan(peer_a(i)))
        pl.semaphore_signal(barrier, inc=1, device_id=to_chan(peer_b(i)))

    @pl.when(me > 0)
    def _():
        pl.semaphore_signal(barrier, inc=1, device_id=to_chan(me - 1))

    @pl.when(me < count - 1)
    def _():
        pl.semaphore_signal(barrier, inc=1, device_id=to_chan(me + 1))

    lane_row = lax.broadcasted_iota(jnp.int32, (1, LANES), 1)
    channel = lax.rem(lane_row, CHANS)

    g[...] = jnp.zeros_like(g)
    y[...] = jnp.zeros_like(y)
    for source, target in ((jones, g), (duals, y)):
        turned = source[...].T
        target[pl.ds(0, STATIONS), :] = turned[:, :LANES]
        target[pl.ds(SIDE, STATIONS), :] = turned[:, LANES:]

    row = lax.broadcasted_iota(jnp.int32, (2 * LANES, LANES), 0)
    lane = lax.broadcasted_iota(jnp.int32, (2 * LANES, LANES), 1)
    mix[...] = jnp.where((row & 67) == (lane & 67), 1.0, 0.0).astype(BF16)

    turned_rows = cbuf.reshape(FULL, 2 * LANES, LANES)
    is_real = (lane_row & 63) < 4
    is_imag = ((lane_row & 63) >= 4) & ((lane_row & 63) < 8)
    blank = jnp.zeros((56, LANES), F32)

    def put(j, coherent, seen):
        rows = pl.ds(LANES * j, LANES)
        turned = coherent.T
        c_real = turned[:, :LANES].astype(F32)
        c_imag = turned[:, LANES:].astype(F32)
        stacked = jnp.concatenate(
            [seen[0:4], seen[8:12], blank, seen[4:8], seen[12:16], blank], axis=0)
        pairs = stacked.T
        seen_real = jnp.where(is_real, pairs, 0.0)
        seen_imag = jnp.where(is_imag, pairs, 0.0)
        if j == FULL:
            live = lax.broadcasted_iota(jnp.int32, (LANES, LANES), 0) < PAIRS - LANES * FULL
            c_real = jnp.where(live, c_real, 0.0)
            c_imag = jnp.where(live, c_imag, 0.0)
            seen_real = jnp.where(live, seen_real, 0.0)
            seen_imag = jnp.where(live, seen_imag, 0.0)
        ct_re[rows, :] = c_real
        ct_im[rows, :] = c_imag
        v_re[rows, :] = seen_real
        v_im[rows, :] = seen_imag

    put(FULL, coh_tail[...].reshape(2 * LANES, LANES), vis_tail[:, 0, :])
    rest = pl.ds(LANES * TILES, FLAT - LANES * TILES)
    for ref in (ct_re, ct_im, v_re, v_im):
        ref[rest, :] = jnp.zeros((FLAT - LANES * TILES, LANES), F32)
    vis_load.wait()
    for j in range(FULL):
        loads[j].wait()
        put(j, turned_rows[j], vbuf[:, LANES * j:LANES * (j + 1)])
    for p in range(STATIONS):
        ct_re[pl.ds(63 * p, 1), :] = jnp.zeros((1, LANES), F32)
        ct_im[pl.ds(63 * p, 1), :] = jnp.zeros((1, LANES), F32)

    def model(block):
        q_real = g[pl.ds(0, SIDE), :]
        q_imag = g[pl.ds(SIDE, SIDE), :]
        left_real, left_imag = [], []
        for i in range(BLOCK):
            p = block * BLOCK + i
            pairs = pl.ds(STATIONS * p, SIDE)
            spot = pl.ds(pl.multiple_of(SIDE * p, SIDE), SIDE)
            c_real = ct_re[pairs, :]
            c_imag = ct_im[pairs, :]
            half_real = c_real * q_real + c_imag * q_imag
            half_imag = c_imag * q_real - c_real * q_imag
            h_re[spot, :] = half_real
            h_im[spot, :] = half_imag
            p_real = g[pl.ds(p, 1), :]
            p_imag = g[pl.ds(SIDE + p, 1), :]
            m_real = (p_real * half_real - p_imag * half_imag) - v_re[pairs, :]
            m_imag = (p_real * half_imag + p_imag * half_real) - v_im[pairs, :]
            for m, left in ((m_real, left_real), (m_imag, left_imag)):
                high = m.astype(BF16)
                left.append(jnp.concatenate([high, (m - high.astype(F32)).astype(BF16)], axis=1))
        spot = pl.ds(pl.multiple_of(ROWS * block, ROWS), ROWS)
        d_re[spot, :] = jnp.dot(jnp.concatenate(left_real, axis=0), mix[...], preferred_element_type=F32)
        d_im[spot, :] = jnp.dot(jnp.concatenate(left_imag, axis=0), mix[...], preferred_element_type=F32)

    def gather_sums(block):
        for i in range(BLOCK):
            p = block * BLOCK + i
            spot = pl.ds(pl.multiple_of(SIDE * p, SIDE), SIDE)
            a, b = h_re[spot, :], h_im[spot, :]
            u, w = d_re[spot, :], d_im[spot, :]
            into = pl.ds(pl.multiple_of(8 * p, 8), 8)

            def folded(x):
                return jnp.sum(x.reshape(8, 8, LANES), axis=0)

            part[0, into, :] = folded(u * a + w * b)
            part[1, into, :] = folded(w * a - u * b)
            part[2, into, :] = folded(a * a + b * b)

    def sums():
        model(0)

        def step(block, carry):
            gather_sums(block - 1)
            model(block)
            return carry

        lax.fori_loop(1, BLOCKS, step, 0)
        gather_sums(BLOCKS - 1)
        out = []
        for i in range(3):
            tiles = []
            for t in range(8):
                total = part[i, pl.ds(64 * t, 8, stride=8), :]
                for s in range(1, 8):
                    total = total + part[i, pl.ds(64 * t + s, 8, stride=8), :]
                tiles.append(total)
            out.append(jnp.concatenate(tiles, axis=0))
        return jnp.concatenate(out[:2], axis=0), jnp.concatenate([out[2], out[2]], axis=0)

    def exchange(turn):
        to_low = pltpu.make_async_remote_copy(
            sent.at[turn], from_high.at[turn], send_low.at[turn], high_sem.at[turn],
            device_id=to_chan(me - 1))
        to_high = pltpu.make_async_remote_copy(
            sent.at[turn], from_low.at[turn], send_high.at[turn], low_sem.at[turn],
            device_id=to_chan(me + 1))
        return to_low, to_high

    def send(turn):
        to_low, to_high = exchange(turn)

        @pl.when(me > 0)
        def _():
            to_low.start()

        @pl.when(me < count - 1)
        def _():
            to_high.start()

    def receive(turn):
        to_low, to_high = exchange(turn)

        @pl.when(me > 0)
        def _():
            to_low.wait_send()
            to_high.wait_recv()

        @pl.when(me < count - 1)
        def _():
            to_high.wait_send()
            to_low.wait_recv()

    def column_sums(x):
        return jnp.sum(x, axis=0, keepdims=True)

    numer, denom = sums()
    gain0 = g[...]
    dual0 = y[...]
    gain1 = (gain0 * denom - numer + penalty * (gain0 - dual0)) / (denom + penalty)
    summed1 = gain1 + dual0
    sent[0] = summed1
    pl.semaphore_wait(barrier, 14 + (me > 0).astype(jnp.int32) + (me < count - 1).astype(jnp.int32))
    send(0)
    z_own = smooth_own(summed1, channel)
    sent[2] = gain0
    g[...] = gain1
    sent[3] = z_own

    numer, denom = sums()
    receive(0)
    gain1 = g[...]
    fresh1 = sent[3] + smooth_sides(from_low[0], from_high[0], channel)
    dual1 = y[...] + gain1 - fresh1
    gain2 = (gain1 * denom - numer + penalty * (fresh1 - dual1)) / (denom + penalty)
    summed2 = gain2 + dual1
    sent[1] = summed2
    send(1)
    gap = gain1 - fresh1
    moved = fresh1 - sent[2]
    first = [column_sums(gap * gap), column_sums(moved * moved) * (penalty * penalty)]
    z_own = smooth_own(summed2, channel)

    def turned_out(x, ref):
        both = jnp.concatenate([x[:SIDE], x[SIDE:]], axis=1).T
        ref[...] = both[:, :STATIONS]

    turned_out(gain2, jones_out)
    receive(1)
    fresh2 = z_own + smooth_sides(from_low[1], from_high[1], channel)
    gap = gain2 - fresh2
    moved = fresh2 - fresh1
    mine[0] = jnp.concatenate(
        first + [column_sums(gap * gap), column_sums(moved * moved) * (penalty * penalty)], axis=0)

    def spread(source, gathered, slot, peer, send_sems, recv_sem):
        copies = []
        for i in range(1, 8):
            copy = pltpu.make_async_remote_copy(
                source, gathered.at[slot], send_sems.at[i], recv_sem, device_id=to_chan(peer(i)))
            copy.start()
            copies.append(copy)
        gathered[slot] = source[...]
        return copies

    def settle(gathered, copies, recv_sem):
        pltpu.make_async_copy(gathered.at[pl.ds(0, 7)], gathered.at[pl.ds(0, 7)], recv_sem).wait()
        for copy in copies:
            copy.wait_send()
        return jnp.sum(gathered[...], axis=0)

    copies = spread(mine.at[0], gather_a, slot_a, peer_a, a_send, a_recv.at[0])
    turned_out(fresh2, cons_out)
    turned_out(dual1 + gain2 - fresh2, duals_out)
    mine[1] = settle(gather_a, copies, a_recv.at[0])
    copies = spread(mine.at[1], gather_b, slot_b, peer_b, b_send, b_recv.at[0])
    total = settle(gather_b, copies, b_recv.at[0])
    total = jnp.sum(total, axis=1, keepdims=True) / entries
    left = lax.broadcasted_iota(jnp.int32, (1, 2), 1) == 0
    norms_out[...] = jnp.concatenate(
        [jnp.where(left, total[0:1], total[1:2]), jnp.where(left, total[2:3], total[3:4])], axis=0)


def local(visibility, coherency, jones_start, duals_start):
    shape = jones_start.shape
    entries = jones_start.size * lax.axis_size("chan")
    vis = visibility.reshape(16, 1, PAIRS)
    coh = coherency.reshape(64, CHANS, PAIRS)
    jones = jones_start.reshape(256, STATIONS)
    duals = duals_start.reshape(256, STATIONS)
    vmem = pl.BlockSpec(memory_space=pltpu.VMEM)
    hbm = pl.BlockSpec(memory_space=pltpu.HBM)
    gains = jax.ShapeDtypeStruct((256, STATIONS), F32)
    pairs = pltpu.VMEM((FLAT, LANES), F32)
    grid_pairs = pltpu.VMEM((SIDE * SIDE, LANES), F32)
    dma = pltpu.SemaphoreType.DMA
    out = pl.pallas_call(
        functools.partial(body, entries=entries),
        grid=(1,),
        out_shape=[gains, gains, gains, jax.ShapeDtypeStruct((2, 2), F32)],
        in_specs=[
            hbm, hbm,
            pl.BlockSpec((16, 1, LANES), lambda i: (0, 0, FULL)),
            pl.BlockSpec((64, CHANS, LANES), lambda i: (0, 0, FULL)),
            vmem, vmem,
        ],
        out_specs=[vmem] * 4,
        scratch_shapes=[
            pltpu.VMEM((FULL, 64, CHANS, LANES), BF16),
            pltpu.VMEM((16, LANES * FULL), F32),
            pairs, pairs, pairs, pairs,
            grid_pairs, grid_pairs, grid_pairs, grid_pairs,
            pltpu.VMEM((2 * LANES, LANES), BF16),
            pltpu.VMEM((2 * SIDE, LANES), F32),
            pltpu.VMEM((2 * SIDE, LANES), F32),
            pltpu.VMEM((3, 8 * SIDE, LANES), F32),
            pltpu.VMEM((4, 2 * SIDE, LANES), F32),
            pltpu.VMEM((2, 2 * SIDE, LANES), F32),
            pltpu.VMEM((2, 2 * SIDE, LANES), F32),
            pltpu.VMEM((2, 4, LANES), F32),
            pltpu.VMEM((8, 4, LANES), F32),
            pltpu.VMEM((8, 4, LANES), F32),
            dma((FULL,)), dma, dma((2,)), dma((2,)), dma((2,)), dma((2,)),
            dma((8,)), dma((1,)), dma((8,)), dma((1,)),
        ],
        compiler_params=pltpu.CompilerParams(
            vmem_limit_bytes=60 * 2**20, collective_id=0, has_side_effects=True),
    )(vis, coh, vis, coh, jones, duals)
    return tuple(part.reshape(shape) for part in out[:3]) + (out[3],)


def solution(mesh):
    gain = P(None, None, "slot", "chan", None)
    return jax.shard_map(
        local,
        mesh=mesh,
        in_specs=(P(None, None, "chan", "slot", None), P(None, None, None, "chan", "slot", None), gain, gain),
        out_specs=(gain, gain, gain, P("slot", None)),
        check_vma=False,
    )
```

```python
import functools

import jax
import jax.numpy as jnp
from jax import lax
from jax.experimental import pallas as pl
from jax.experimental.pallas import tpu as pltpu
from jax.sharding import PartitionSpec as P

STATIONS = 62
SIDE = 64
CHANS = 4
PAIRS = STATIONS * STATIONS
LANES = 128
FULL = PAIRS // LANES
TILES = FULL + 1
FLAT = STATIONS * SIDE + 2 * SIDE
BLOCK = 4
BLOCKS = SIDE // BLOCK
ROWS = BLOCK * SIDE
GROUP = 8
VMEM_LIMIT = 65_500_000

penalty = 8.0
kernel_taps = (0.04, 0.06, 0.1, 0.15, 0.3, 0.15, 0.1, 0.06, 0.04)
F32 = jnp.float32
BF16 = jnp.bfloat16


def to_chan(index):
    return {"chan": index}


def shifted(x, by):
    return x if by == 0 else pltpu.roll(x, (-by) % LANES, axis=1)


def smooth_own(own, channel):
    total = None
    for o in range(-3, 4):
        weight = jnp.where((channel + o >= 0) & (channel + o < CHANS), kernel_taps[o + 4], 0.0)
        term = shifted(own, o) * weight
        total = term if total is None else total + term
    return total


def smooth_sides(low, high, channel):
    total = None
    for o in range(1, 5):
        weight = jnp.where(channel - o < 0, kernel_taps[4 - o], 0.0)
        term = shifted(low, CHANS - o) * weight
        total = term if total is None else total + term
        weight = jnp.where(channel + o >= CHANS, kernel_taps[4 + o], 0.0)
        total = total + shifted(high, o - CHANS) * weight
    return total


def body(
    vis, coh, vis_tail, coh_tail, jones, duals,
    jones_out, cons_out, duals_out, norms_out,
    cbuf, vbuf, ct_re, ct_im, v_re, v_im, h_re, h_im, d_re, d_im, mix,
    g, y, part, left, sent, from_low, from_high, mine, gathered,
    load_sems, vis_sem, send_low, send_high, low_sem, high_sem,
    norm_send, norm_recv,
    *, entries,
):
    count = lax.axis_size("chan")
    me = lax.axis_index("chan")
    loads = []
    for first in range(0, FULL, GROUP):
        size = min(GROUP, FULL - first)
        sem = load_sems.at[first // GROUP]
        for j in range(first, first + size):
            pltpu.make_async_copy(
                coh.at[:, :, pl.ds(LANES * j, LANES)], cbuf.at[j], sem).start()
        span = cbuf.at[pl.ds(first, size)]
        loads.append((first, size, pltpu.make_async_copy(span, span, sem)))
    vis_load = pltpu.make_async_copy(
        vis.at[:, 0, pl.ds(0, LANES * FULL)], vbuf, vis_sem)
    vis_load.start()

    @pl.when(me == 0)
    def _():
        from_low[...] = jnp.zeros_like(from_low)

    @pl.when(me == count - 1)
    def _():
        from_high[...] = jnp.zeros_like(from_high)

    barrier = pltpu.get_barrier_semaphore()

    @pl.loop(1, count)
    def _(i):
        pl.semaphore_signal(barrier, inc=1, device_id=to_chan(lax.rem(me + i, count)))

    lane_row = lax.broadcasted_iota(jnp.int32, (1, LANES), 1)
    channel = lax.rem(lane_row, CHANS)

    g[...] = jnp.zeros_like(g)
    y[...] = jnp.zeros_like(y)
    for source, target in ((jones, g), (duals, y)):
        turned = source[...].T
        target[pl.ds(0, STATIONS), :] = turned[:, :LANES]
        target[pl.ds(SIDE, STATIONS), :] = turned[:, LANES:]

    row = lax.broadcasted_iota(jnp.int32, (2 * LANES, LANES), 0)
    lane = lax.broadcasted_iota(jnp.int32, (2 * LANES, LANES), 1)
    mix[...] = jnp.where((row & 67) == (lane & 67), 1.0, 0.0).astype(BF16)

    turned_rows = cbuf.reshape(FULL, 2 * LANES, LANES)
    place = (lane_row & 63) // CHANS
    vis_load.wait()

    def put(j, coherent, pairs):
        rows = pl.ds(LANES * j, LANES)
        turned = coherent.T
        values = [
            turned[:, :LANES].astype(F32),
            turned[:, LANES:].astype(F32),
            jnp.where(place == 2 * (j % GROUP), pairs, 0.0),
            jnp.where(place == 2 * (j % GROUP) + 1, pairs, 0.0),
        ]
        for ref, value in zip((ct_re, ct_im, v_re, v_im), values):
            if j == FULL:
                live = lax.broadcasted_iota(jnp.int32, (LANES, LANES), 0) < PAIRS - LANES * FULL
                value = jnp.where(live, value, 0.0)
            ref[rows, :] = value

    rest = pl.ds(LANES * TILES, FLAT - LANES * TILES)
    for ref in (ct_re, ct_im, v_re, v_im):
        ref[rest, :] = jnp.zeros((FLAT - LANES * TILES, LANES), F32)
    for first, size, load in loads:
        load.wait()
        seen = [vbuf[:, LANES * j:LANES * (j + 1)] for j in range(first, first + size)]
        if first + size == FULL:
            seen.append(vis_tail[:, 0, :])
        halves = []
        for pol in range(2):
            for each in seen:
                halves += [each[4 * pol:4 * pol + 4], each[8 + 4 * pol:12 + 4 * pol]]
            if len(seen) < GROUP:
                halves.append(jnp.zeros((8 * (GROUP - len(seen)), LANES), F32))
        pairs = jnp.concatenate(halves, axis=0).T
        for j in range(first, first + size):
            put(j, turned_rows[j], pairs)
        if first + size == FULL:
            put(FULL, coh_tail[...].reshape(2 * LANES, LANES), pairs)
    for p in range(STATIONS):
        ct_re[pl.ds(63 * p, 1), :] = jnp.zeros((1, LANES), F32)
        ct_im[pl.ds(63 * p, 1), :] = jnp.zeros((1, LANES), F32)

    def model(block):
        q_real = g[pl.ds(0, SIDE), :]
        q_imag = g[pl.ds(SIDE, SIDE), :]
        for i in range(BLOCK):
            p = block * BLOCK + i
            pairs = pl.ds(STATIONS * p, SIDE)
            spot = pl.ds(pl.multiple_of(SIDE * p, SIDE), SIDE)
            c_real = ct_re[pairs, :]
            c_imag = ct_im[pairs, :]
            half_real = c_real * q_real + c_imag * q_imag
            half_imag = c_imag * q_real - c_real * q_imag
            h_re[spot, :] = half_real
            h_im[spot, :] = half_imag
            p_real = g[pl.ds(p, 1), :]
            p_imag = g[pl.ds(SIDE + p, 1), :]
            m_real = (p_real * half_real - p_imag * half_imag) - v_re[pairs, :]
            m_imag = (p_real * half_imag + p_imag * half_real) - v_im[pairs, :]
            for side, m in enumerate((m_real, m_imag)):
                high = m.astype(BF16)
                left[side, spot, :LANES] = high
                left[side, spot, LANES:] = (m - high.astype(F32)).astype(BF16)

    def lane_sums(block):
        spot = pl.ds(pl.multiple_of(ROWS * block, ROWS), ROWS)
        d_re[spot, :] = jnp.dot(left[0, spot, :], mix[...], preferred_element_type=F32)
        d_im[spot, :] = jnp.dot(left[1, spot, :], mix[...], preferred_element_type=F32)

    def gather_sums(block):
        for i in range(BLOCK):
            p = block * BLOCK + i
            spot = pl.ds(pl.multiple_of(SIDE * p, SIDE), SIDE)
            a, b = h_re[spot, :], h_im[spot, :]
            u, w = d_re[spot, :], d_im[spot, :]
            into = pl.ds(pl.multiple_of(8 * p, 8), 8)

            def folded(x):
                return jnp.sum(x.reshape(8, 8, LANES), axis=0)

            part[0, into, :] = folded(u * a + w * b)
            part[1, into, :] = folded(w * a - u * b)
            part[2, into, :] = folded(a * a + b * b)

    def sums():
        model(0)
        lane_sums(0)
        model(1)

        def step(block, carry):
            gather_sums(block - 2)
            lane_sums(block - 1)
            model(block)
            return carry

        lax.fori_loop(2, BLOCKS, step, 0)
        gather_sums(BLOCKS - 2)
        lane_sums(BLOCKS - 1)
        gather_sums(BLOCKS - 1)
        out = []
        for i in range(3):
            tiles = []
            for t in range(8):
                total = part[i, pl.ds(64 * t, 8, stride=8), :]
                for s in range(1, 8):
                    total = total + part[i, pl.ds(64 * t + s, 8, stride=8), :]
                tiles.append(total)
            out.append(jnp.concatenate(tiles, axis=0))
        return jnp.concatenate(out[:2], axis=0), jnp.concatenate([out[2], out[2]], axis=0)

    def exchange(turn):
        to_low = pltpu.make_async_remote_copy(
            sent.at[turn], from_high.at[turn], send_low.at[turn], high_sem.at[turn],
            device_id=to_chan(me - 1))
        to_high = pltpu.make_async_remote_copy(
            sent.at[turn], from_low.at[turn], send_high.at[turn], low_sem.at[turn],
            device_id=to_chan(me + 1))
        return to_low, to_high

    def send(turn):
        to_low, to_high = exchange(turn)

        @pl.when(me > 0)
        def _():
            to_low.start()

        @pl.when(me < count - 1)
        def _():
            to_high.start()

    def receive(turn):
        to_low, to_high = exchange(turn)

        @pl.when(me > 0)
        def _():
            to_low.wait_send()
            to_high.wait_recv()

        @pl.when(me < count - 1)
        def _():
            to_high.wait_send()
            to_low.wait_recv()

    def column_sums(x):
        return jnp.sum(x, axis=0, keepdims=True)

    numer, denom = sums()
    gain0 = g[...]
    dual0 = y[...]
    gain1 = (gain0 * denom - numer + penalty * (gain0 - dual0)) / (denom + penalty)
    summed1 = gain1 + dual0
    sent[0] = summed1
    pl.semaphore_wait(barrier, count - 1)
    send(0)
    z_own = smooth_own(summed1, channel)
    sent[2] = gain0
    g[...] = gain1
    sent[3] = z_own

    numer, denom = sums()
    receive(0)
    gain1 = g[...]
    fresh1 = sent[3] + smooth_sides(from_low[0], from_high[0], channel)
    dual1 = y[...] + gain1 - fresh1
    gain2 = (gain1 * denom - numer + penalty * (fresh1 - dual1)) / (denom + penalty)
    summed2 = gain2 + dual1
    sent[1] = summed2
    send(1)
    gap = gain1 - fresh1
    moved = fresh1 - sent[2]
    first = [column_sums(gap * gap), column_sums(moved * moved) * (penalty * penalty)]
    z_own = smooth_own(summed2, channel)

    def turned_out(x, ref):
        both = jnp.concatenate([x[:SIDE], x[SIDE:]], axis=1).T
        ref[...] = both[:, :STATIONS]

    turned_out(gain2, jones_out)
    receive(1)
    fresh2 = z_own + smooth_sides(from_low[1], from_high[1], channel)
    gap = gain2 - fresh2
    moved = fresh2 - fresh1
    four = jnp.concatenate(
        first + [column_sums(gap * gap), column_sums(moved * moved) * (penalty * penalty)], axis=0)
    four = jnp.sum(four, axis=1, keepdims=True)
    own_lane = lax.broadcasted_iota(jnp.int32, (4, LANES), 0) == lax.broadcasted_iota(
        jnp.int32, (4, LANES), 1)
    mine[...] = jnp.sum(jnp.where(own_lane, four, 0.0), axis=0, keepdims=True)

    def to_peer(i):
        return pltpu.make_async_remote_copy(
            mine, gathered.at[me], norm_send, norm_recv,
            device_id=to_chan(lax.rem(me + i, count)))

    @pl.loop(1, count)
    def _(i):
        to_peer(i).start()

    gathered[me] = mine[...]
    turned_out(fresh2, cons_out)
    turned_out(dual1 + gain2 - fresh2, duals_out)
    others = gathered.at[pl.ds(0, count - 1)]
    pltpu.make_async_copy(others, others, norm_recv).wait()
    pltpu.make_async_copy(others, others, norm_send).wait()
    total = jnp.sum(gathered[...], axis=0) / entries
    norms_out[...] = jnp.concatenate(
        [total[:, :2], pltpu.roll(total, LANES - 2, axis=1)[:, :2]], axis=0)


def write_out(*refs):
    sems = refs[-1]
    into = [pltpu.make_async_copy(refs[i], refs[8 + i], sems.at[i]) for i in range(4)]
    onward = [pltpu.make_async_copy(refs[8 + i], refs[4 + i], sems.at[i]) for i in range(4)]
    for copy in into:
        copy.start()
    for first, second in zip(into, onward):
        first.wait()
        second.start()
    for copy in onward:
        copy.wait()


def local(visibility, coherency, jones_start, duals_start):
    shape = jones_start.shape
    entries = jones_start.size * lax.axis_size("chan")
    vis = visibility.reshape(16, 1, PAIRS)
    coh = coherency.reshape(64, CHANS, PAIRS)
    jones = jones_start.reshape(256, STATIONS)
    duals = duals_start.reshape(256, STATIONS)
    vmem = pl.BlockSpec(memory_space=pltpu.VMEM)
    hbm = pl.BlockSpec(memory_space=pltpu.HBM)
    gains = jax.ShapeDtypeStruct((256, STATIONS), F32)
    pairs = pltpu.VMEM((FLAT, LANES), F32)
    grid_pairs = pltpu.VMEM((SIDE * SIDE, LANES), F32)
    dma = pltpu.SemaphoreType.DMA
    out = pl.pallas_call(
        functools.partial(body, entries=entries),
        grid=(1,),
        out_shape=[gains, gains, gains, jax.ShapeDtypeStruct((2, 2), F32)],
        in_specs=[
            hbm, hbm,
            pl.BlockSpec((16, 1, LANES), lambda i: (0, 0, FULL)),
            pl.BlockSpec((64, CHANS, LANES), lambda i: (0, 0, FULL)),
            vmem, vmem,
        ],
        out_specs=[vmem] * 4,
        scratch_shapes=[
            pltpu.VMEM((FULL, 64, CHANS, LANES), BF16),
            pltpu.VMEM((16, LANES * FULL), F32),
            pairs, pairs, pairs, pairs,
            grid_pairs, grid_pairs, grid_pairs, grid_pairs,
            pltpu.VMEM((2 * LANES, LANES), BF16),
            pltpu.VMEM((2 * SIDE, LANES), F32),
            pltpu.VMEM((2 * SIDE, LANES), F32),
            pltpu.VMEM((3, 8 * SIDE, LANES), F32),
            pltpu.VMEM((2, SIDE * SIDE, 2 * LANES), BF16),
            pltpu.VMEM((4, 2 * SIDE, LANES), F32),
            pltpu.VMEM((2, 2 * SIDE, LANES), F32),
            pltpu.VMEM((2, 2 * SIDE, LANES), F32),
            pltpu.VMEM((1, LANES), F32),
            pltpu.VMEM((lax.axis_size("chan"), 1, LANES), F32),
            dma((-(-FULL // GROUP),)), dma, dma((2,)), dma((2,)), dma((2,)), dma((2,)),
            dma, dma,
        ],
        compiler_params=pltpu.CompilerParams(
            vmem_limit_bytes=VMEM_LIMIT, collective_id=0, has_side_effects=True),
    )(vis, coh, vis, coh, jones, duals)
    anywhere = pl.BlockSpec(memory_space=pl.ANY)
    out = pl.pallas_call(
        write_out,
        out_shape=[jax.ShapeDtypeStruct(part.shape, part.dtype) for part in out],
        in_specs=[anywhere] * 4,
        out_specs=[anywhere] * 4,
        scratch_shapes=[pltpu.VMEM(part.shape, part.dtype) for part in out] + [dma((4,))],
    )(*out)
    return tuple(part.reshape(shape) for part in out[:3]) + (out[3],)


def solution(mesh):
    gain = P(None, None, "slot", "chan", None)
    return jax.shard_map(
        local,
        mesh=mesh,
        in_specs=(P(None, None, "chan", "slot", None), P(None, None, None, "chan", "slot", None), gain, gain),
        out_specs=(gain, gain, gain, P("slot", None)),
        check_vma=False,
    )
```

```python
import functools

import jax
import jax.numpy as jnp
from jax import lax
from jax.experimental import pallas as pl
from jax.experimental.pallas import tpu as pltpu
from jax.sharding import PartitionSpec as P

STATIONS = 62
SIDE = 64
CHANS = 4
PAIRS = STATIONS * STATIONS
LANES = 128
FULL = PAIRS // LANES
TILES = FULL + 1
FLAT = STATIONS * SIDE + 2 * SIDE
BLOCK = 31
BLOCKS = STATIONS // BLOCK
GROUP = 8
DOT = 4
STEP = 16
VMEM_LIMIT = 65_500_000

penalty = 8.0
kernel_taps = (0.04, 0.06, 0.1, 0.15, 0.3, 0.15, 0.1, 0.06, 0.04)
F32 = jnp.float32
BF16 = jnp.bfloat16


def to_chan(index):
    return {"chan": index}


def shifted(x, by):
    return x if by == 0 else pltpu.roll(x, (-by) % LANES, axis=1)


def smooth_own(own, channel):
    total = None
    for o in range(-3, 4):
        weight = jnp.where((channel + o >= 0) & (channel + o < CHANS), kernel_taps[o + 4], 0.0)
        term = shifted(own, o) * weight
        total = term if total is None else total + term
    return total


def smooth_sides(low, high, channel):
    total = None
    for o in range(1, 5):
        weight = jnp.where(channel - o < 0, kernel_taps[4 - o], 0.0)
        term = shifted(low, CHANS - o) * weight
        total = term if total is None else total + term
        weight = jnp.where(channel + o >= CHANS, kernel_taps[4 + o], 0.0)
        total = total + shifted(high, o - CHANS) * weight
    return total


def body(
    vis, coh, jones_in, duals_in,
    jones_out, cons_out, duals_out, norms_out,
    gains_buf, norms_buf, out_sems,
    jones, duals, vis_tail, coh_tail, in_sems,
    cbuf, vbuf, ct_re, ct_im, v_re, v_im, h_re, h_im, mix,
    g, y, part, sent, from_low, from_high, mine, gathered,
    load_sems, vis_sem, send_low, send_high, low_sem, high_sem,
    norm_send, norm_recv,
    *, entries,
):
    count = lax.axis_size("chan")
    me = lax.axis_index("chan")
    loads = []
    for first in range(0, FULL, GROUP):
        size = min(GROUP, FULL - first)
        sem = load_sems.at[first // GROUP]
        for j in range(first, first + size):
            pltpu.make_async_copy(
                coh.at[:, :, pl.ds(LANES * j, LANES)], cbuf.at[j], sem).start()
        span = cbuf.at[pl.ds(first, size)]
        loads.append((first, size, pltpu.make_async_copy(span, span, sem)))
    vis_load = pltpu.make_async_copy(
        vis.at[:, 0, pl.ds(0, LANES * FULL)], vbuf, vis_sem)
    vis_load.start()
    ends = pl.ds(LANES * (FULL - 1), PAIRS - LANES * (FULL - 1))
    small = [
        pltpu.make_async_copy(jones_in, jones, in_sems.at[0]),
        pltpu.make_async_copy(duals_in, duals, in_sems.at[1]),
        pltpu.make_async_copy(vis.at[:, :, ends], vis_tail, in_sems.at[2]),
        pltpu.make_async_copy(coh.at[:, :, ends], coh_tail, in_sems.at[3]),
    ]
    for copy in small:
        copy.start()

    @pl.when(me == 0)
    def _():
        from_low[...] = jnp.zeros_like(from_low)

    @pl.when(me == count - 1)
    def _():
        from_high[...] = jnp.zeros_like(from_high)

    barrier = pltpu.get_barrier_semaphore()

    @pl.loop(1, count)
    def _(i):
        pl.semaphore_signal(barrier, inc=1, device_id=to_chan(lax.rem(me + i, count)))

    lane_row = lax.broadcasted_iota(jnp.int32, (1, LANES), 1)
    channel = lax.rem(lane_row, CHANS)

    for ref in (g, y, part):
        ref[...] = jnp.zeros_like(ref)
    for copy in small:
        copy.wait()
    for source, target in ((jones, g), (duals, y)):
        turned = source[...].T
        target[pl.ds(0, STATIONS), :] = turned[:, :LANES]
        target[pl.ds(SIDE, STATIONS), :] = turned[:, LANES:]

    row = lax.broadcasted_iota(jnp.int32, (2 * LANES, 2 * LANES), 0)
    lane = lax.broadcasted_iota(jnp.int32, (2 * LANES, 2 * LANES), 1)
    mix[...] = jnp.where((row & 195) == (lane & 195), 1.0, 0.0).astype(BF16)

    turned_rows = cbuf.reshape(FULL, 2 * LANES, LANES)
    place = (lane_row & 63) // CHANS
    vis_load.wait()

    def put(j, coherent, pairs):
        rows = pl.ds(LANES * j, LANES)
        turned = coherent.T
        values = [
            turned[:, :LANES].astype(F32),
            turned[:, LANES:].astype(F32),
            jnp.where(place == 2 * (j % GROUP), pairs, 0.0),
            jnp.where(place == 2 * (j % GROUP) + 1, pairs, 0.0),
        ]
        for ref, value in zip((ct_re, ct_im, v_re, v_im), values):
            if j == FULL:
                live = lax.broadcasted_iota(jnp.int32, (LANES, LANES), 0) < PAIRS - LANES * FULL
                value = jnp.where(live, value, 0.0)
            ref[rows, :] = value

    rest = pl.ds(LANES * TILES, FLAT - LANES * TILES)
    for ref in (ct_re, ct_im, v_re, v_im):
        ref[rest, :] = jnp.zeros((FLAT - LANES * TILES, LANES), F32)
    for first, size, load in loads:
        load.wait()
        seen = [vbuf[:, LANES * j:LANES * (j + 1)] for j in range(first, first + size)]
        if first + size == FULL:
            seen.append(jnp.concatenate(
                [vis_tail[:, 0, LANES:], jnp.zeros((16, 2 * LANES - vis_tail.shape[2]), F32)], axis=1))
        halves = []
        for pol in range(2):
            for each in seen:
                halves += [each[4 * pol:4 * pol + 4], each[8 + 4 * pol:12 + 4 * pol]]
            if len(seen) < GROUP:
                halves.append(jnp.zeros((8 * (GROUP - len(seen)), LANES), F32))
        pairs = jnp.concatenate(halves, axis=0).T
        for j in range(first, first + size):
            put(j, turned_rows[j], pairs)
        if first + size == FULL:
            put(FULL, jnp.concatenate(
                [coh_tail[:, :, LANES:], jnp.zeros((64, CHANS, 2 * LANES - coh_tail.shape[2]), BF16)],
                axis=2).reshape(2 * LANES, LANES), pairs)
    for p in range(STATIONS):
        ct_re[pl.ds(63 * p, 1), :] = jnp.zeros((1, LANES), F32)
        ct_im[pl.ds(63 * p, 1), :] = jnp.zeros((1, LANES), F32)

    def model(p):
        p_real = jnp.broadcast_to(g[pl.ds(p, 1), :], (STEP, LANES))
        p_imag = jnp.broadcast_to(g[pl.ds(SIDE + p, 1), :], (STEP, LANES))
        highs, lows = [], []
        for q in range(0, SIDE, STEP):
            pairs = pl.ds(STATIONS * p + q, STEP)
            q_real = g[pl.ds(q, STEP), :]
            q_imag = g[pl.ds(SIDE + q, STEP), :]
            c_real = ct_re[pairs, :]
            c_imag = ct_im[pairs, :]
            half_real = c_real * q_real + c_imag * q_imag
            half_imag = c_imag * q_real - c_real * q_imag
            spot = pl.ds(pl.multiple_of(SIDE * p + q, STEP), STEP)
            h_re[spot, :] = half_real
            h_im[spot, :] = half_imag
            m_real = (p_real * half_real - p_imag * half_imag) - v_re[pairs, :]
            m_imag = (p_real * half_imag + p_imag * half_real) - v_im[pairs, :]
            m = jnp.concatenate([m_real, m_imag], axis=1)
            high = m.astype(BF16)
            highs.append(high)
            lows.append((m - high.astype(F32)).astype(BF16))
        return highs, lows

    def gather_sums(p, sums):
        total = None
        for q in range(0, SIDE, 8):
            spot = pl.ds(pl.multiple_of(SIDE * p + q, 8), 8)
            a, b = h_re[spot, :], h_im[spot, :]
            u, w = sums[q:q + 8, :LANES], sums[q:q + 8, LANES:]
            three = (u * a + w * b, w * a - u * b, a * a + b * b)
            total = three if total is None else [x + y for x, y in zip(total, three)]
        into = pl.ds(pl.multiple_of(8 * p, 8), 8)
        for i in range(3):
            part[i, into, :] = total[i]

    def sums():
        def step(block, carry):
            held = []
            for first in range(0, BLOCK, DOT):
                size = min(DOT, BLOCK - first)
                stations = [block * BLOCK + first + i for i in range(size)]
                models = [model(p) for p in stations]
                lhs = jnp.concatenate(
                    [x for side in (0, 1) for each in models for x in each[side]], axis=0)
                dot = jnp.dot(lhs, mix[...], preferred_element_type=F32)
                total = dot[:SIDE * size] + dot[SIDE * size:]
                held.append((stations, total))
            for stations, total in held:
                for i, p in enumerate(stations):
                    gather_sums(p, total[SIDE * i:SIDE * (i + 1)])
            return carry

        lax.fori_loop(0, BLOCKS, step, 0)
        out = []
        for i in range(3):
            tiles = []
            for t in range(8):
                total = part[i, pl.ds(64 * t, 8, stride=8), :]
                for s in range(1, 8):
                    total = total + part[i, pl.ds(64 * t + s, 8, stride=8), :]
                tiles.append(total)
            out.append(jnp.concatenate(tiles, axis=0))
        return jnp.concatenate(out[:2], axis=0), jnp.concatenate([out[2], out[2]], axis=0)

    def exchange(turn):
        to_low = pltpu.make_async_remote_copy(
            sent.at[turn], from_high.at[turn], send_low.at[turn], high_sem.at[turn],
            device_id=to_chan(me - 1))
        to_high = pltpu.make_async_remote_copy(
            sent.at[turn], from_low.at[turn], send_high.at[turn], low_sem.at[turn],
            device_id=to_chan(me + 1))
        return to_low, to_high

    def send(turn):
        to_low, to_high = exchange(turn)

        @pl.when(me > 0)
        def _():
            to_low.start()

        @pl.when(me < count - 1)
        def _():
            to_high.start()

    def receive(turn):
        to_low, to_high = exchange(turn)

        @pl.when(me > 0)
        def _():
            to_low.wait_send()
            to_high.wait_recv()

        @pl.when(me < count - 1)
        def _():
            to_high.wait_send()
            to_low.wait_recv()

    def column_sums(x):
        return jnp.sum(x, axis=0, keepdims=True)

    numer, denom = sums()
    gain0 = g[...]
    dual0 = y[...]
    gain1 = (gain0 * denom - numer + penalty * (gain0 - dual0)) / (denom + penalty)
    summed1 = gain1 + dual0
    sent[0] = summed1
    pl.semaphore_wait(barrier, count - 1)
    send(0)
    z_own = smooth_own(summed1, channel)
    sent[2] = gain0
    g[...] = gain1
    sent[3] = z_own

    numer, denom = sums()
    receive(0)
    gain1 = g[...]
    fresh1 = sent[3] + smooth_sides(from_low[0], from_high[0], channel)
    dual1 = y[...] + gain1 - fresh1
    gain2 = (gain1 * denom - numer + penalty * (fresh1 - dual1)) / (denom + penalty)
    summed2 = gain2 + dual1
    sent[1] = summed2
    send(1)
    gap = gain1 - fresh1
    moved = fresh1 - sent[2]
    first = [column_sums(gap * gap), column_sums(moved * moved) * (penalty * penalty)]
    z_own = smooth_own(summed2, channel)

    outs = []

    def turned_out(x, ref):
        both = jnp.concatenate([x[:SIDE], x[SIDE:]], axis=1).T
        at = len(outs)
        gains_buf[at] = both[:, :STATIONS]
        outs.append(pltpu.make_async_copy(gains_buf.at[at], ref, out_sems.at[at]))
        outs[-1].start()

    turned_out(gain2, jones_out)
    receive(1)
    fresh2 = z_own + smooth_sides(from_low[1], from_high[1], channel)
    gap = gain2 - fresh2
    moved = fresh2 - fresh1
    four = jnp.concatenate(
        first + [column_sums(gap * gap), column_sums(moved * moved) * (penalty * penalty)], axis=0)
    four = jnp.sum(four, axis=1, keepdims=True)
    own_lane = lax.broadcasted_iota(jnp.int32, (4, LANES), 0) == lax.broadcasted_iota(
        jnp.int32, (4, LANES), 1)
    mine[...] = jnp.sum(jnp.where(own_lane, four, 0.0), axis=0, keepdims=True)

    @pl.loop(0, count)
    def _(i):
        peer = lax.rem(i, 8) // 2 * 16 + i // 8 * 2 + lax.rem(i, 2)

        @pl.when(peer != me)
        def _():
            pltpu.make_async_remote_copy(
                mine, gathered.at[me], norm_send, norm_recv, device_id=to_chan(peer)).start()

    gathered[me] = mine[...]
    turned_out(fresh2, cons_out)
    turned_out(dual1 + gain2 - fresh2, duals_out)
    others = gathered.at[pl.ds(0, count - 1)]
    pltpu.make_async_copy(others, others, norm_recv).wait()
    pltpu.make_async_copy(others, others, norm_send).wait()
    total = jnp.sum(gathered[...], axis=0) / entries
    norms_buf[...] = jnp.concatenate(
        [total[:, :2], pltpu.roll(total, LANES - 2, axis=1)[:, :2]], axis=0)
    outs.append(pltpu.make_async_copy(norms_buf, norms_out, out_sems.at[3]))
    outs[-1].start()
    for copy in outs:
        copy.wait()


def write_out(*refs):
    sems = refs[-1]
    into = [pltpu.make_async_copy(refs[i], refs[8 + i], sems.at[i]) for i in range(4)]
    onward = [pltpu.make_async_copy(refs[8 + i], refs[4 + i], sems.at[i]) for i in range(4)]
    for copy in into:
        copy.start()
    for first, second in zip(into, onward):
        first.wait()
        second.start()
    for copy in onward:
        copy.wait()


def local(visibility, coherency, jones_start, duals_start):
    shape = jones_start.shape
    entries = jones_start.size * lax.axis_size("chan")
    vis = visibility.reshape(16, 1, PAIRS)
    coh = coherency.reshape(64, CHANS, PAIRS)
    jones = jones_start.reshape(256, STATIONS)
    duals = duals_start.reshape(256, STATIONS)
    hbm = pl.BlockSpec(memory_space=pltpu.HBM)
    gains = jax.ShapeDtypeStruct((256, STATIONS), F32)
    pairs = pltpu.VMEM((FLAT, LANES), F32)
    grid_pairs = pltpu.VMEM((SIDE * SIDE, LANES), F32)
    dma = pltpu.SemaphoreType.DMA
    out = pl.pallas_call(
        functools.partial(body, entries=entries),
        out_shape=[gains, gains, gains, jax.ShapeDtypeStruct((2, 2), F32)],
        in_specs=[hbm] * 4,
        out_specs=[hbm] * 4,
        scratch_shapes=[
            pltpu.VMEM((3, 256, STATIONS), F32),
            pltpu.VMEM((2, 2), F32),
            dma((4,)),
            pltpu.VMEM((256, STATIONS), F32),
            pltpu.VMEM((256, STATIONS), F32),
            pltpu.VMEM((16, 1, PAIRS - LANES * (FULL - 1)), F32),
            pltpu.VMEM((64, CHANS, PAIRS - LANES * (FULL - 1)), BF16),
            dma((4,)),
            pltpu.VMEM((FULL, 64, CHANS, LANES), BF16),
            pltpu.VMEM((16, LANES * FULL), F32),
            pairs, pairs, pairs, pairs,
            grid_pairs, grid_pairs,
            pltpu.VMEM((2 * LANES, 2 * LANES), BF16),
            pltpu.VMEM((2 * SIDE, LANES), F32),
            pltpu.VMEM((2 * SIDE, LANES), F32),
            pltpu.VMEM((3, 8 * SIDE, LANES), F32),
            pltpu.VMEM((4, 2 * SIDE, LANES), F32),
            pltpu.VMEM((2, 2 * SIDE, LANES), F32),
            pltpu.VMEM((2, 2 * SIDE, LANES), F32),
            pltpu.VMEM((1, LANES), F32),
            pltpu.VMEM((lax.axis_size("chan"), 1, LANES), F32),
            dma((-(-FULL // GROUP),)), dma, dma((2,)), dma((2,)), dma((2,)), dma((2,)),
            dma, dma,
        ],
        compiler_params=pltpu.CompilerParams(
            vmem_limit_bytes=VMEM_LIMIT, collective_id=0, has_side_effects=True),
    )(vis, coh, jones, duals)
    anywhere = pl.BlockSpec(memory_space=pl.ANY)
    out = pl.pallas_call(
        write_out,
        out_shape=[jax.ShapeDtypeStruct(part.shape, part.dtype) for part in out],
        in_specs=[anywhere] * 4,
        out_specs=[anywhere] * 4,
        scratch_shapes=[pltpu.VMEM(part.shape, part.dtype) for part in out] + [dma((4,))],
    )(*out)
    return tuple(part.reshape(shape) for part in out[:3]) + (out[3],)


def solution(mesh):
    gain = P(None, None, "slot", "chan", None)
    return jax.shard_map(
        local,
        mesh=mesh,
        in_specs=(P(None, None, "chan", "slot", None), P(None, None, None, "chan", "slot", None), gain, gain),
        out_specs=(gain, gain, gain, P("slot", None)),
        check_vma=False,
    )
```

```python
import functools

import jax
import jax.numpy as jnp
from jax import lax
from jax.experimental import pallas as pl
from jax.experimental.pallas import tpu as pltpu
from jax.sharding import PartitionSpec as P

STATIONS = 62
SIDE = 64
CHANS = 4
PAIRS = STATIONS * STATIONS
LANES = 128
FULL = PAIRS // LANES
TILES = FULL + 1
FLAT = STATIONS * SIDE + 2 * SIDE
HALF = SIDE // 2
GROUP = 8
DOT = 2
STEP = 16
VMEM_LIMIT = 65_500_000

penalty = 8.0
kernel_taps = (0.04, 0.06, 0.1, 0.15, 0.3, 0.15, 0.1, 0.06, 0.04)
F32 = jnp.float32
BF16 = jnp.bfloat16


def to_chan(index):
    return {"chan": index}


def shifted(x, by):
    return x if by == 0 else pltpu.roll(x, (-by) % LANES, axis=1)


def smooth_own(own, channel):
    total = None
    for o in range(-3, 4):
        weight = jnp.where((channel + o >= 0) & (channel + o < CHANS), kernel_taps[o + 4], 0.0)
        term = shifted(own, o) * weight
        total = term if total is None else total + term
    return total


def smooth_sides(low, high, channel):
    total = None
    for o in range(1, 5):
        weight = jnp.where(channel - o < 0, kernel_taps[4 - o], 0.0)
        term = shifted(low, CHANS - o) * weight
        total = term if total is None else total + term
        weight = jnp.where(channel + o >= CHANS, kernel_taps[4 + o], 0.0)
        total = total + shifted(high, o - CHANS) * weight
    return total


def body(
    vis, coh, jones_in, duals_in,
    jones_out, cons_out, duals_out, norms_out,
    gains_buf, norms_buf, out_sems,
    jones, duals, vis_tail, coh_tail, in_sems,
    cbuf, vbuf, ct_re, ct_im, v_re, v_im, h_re, h_im, mix,
    g, y, part, kept, sent, from_low, from_high, mine, gathered,
    load_sems, vis_sem, send_low, send_high, low_sem, high_sem,
    norm_send, norm_recv,
    *, entries,
):
    count = lax.axis_size("chan")
    me = lax.axis_index("chan")
    nought = lax.div(me, 1024)
    loads = []
    for first in range(0, FULL, GROUP):
        size = min(GROUP, FULL - first)
        sem = load_sems.at[first // GROUP]
        for j in range(first, first + size):
            pltpu.make_async_copy(
                coh.at[:, :, pl.ds(LANES * j, LANES)], cbuf.at[j], sem).start()
        span = cbuf.at[pl.ds(first, size)]
        loads.append((first, size, pltpu.make_async_copy(span, span, sem)))
        if first == 0:
            vis_load = pltpu.make_async_copy(
                vis.at[:, 0, pl.ds(0, LANES * FULL)], vbuf, vis_sem)
            vis_load.start()
            ends = pl.ds(LANES * (FULL - 1), PAIRS - LANES * (FULL - 1))
            small = [
                pltpu.make_async_copy(jones_in, jones, in_sems.at[0]),
                pltpu.make_async_copy(duals_in, duals, in_sems.at[1]),
                pltpu.make_async_copy(vis.at[:, :, ends], vis_tail, in_sems.at[2]),
                pltpu.make_async_copy(coh.at[:, :, ends], coh_tail, in_sems.at[3]),
            ]
            for copy in small:
                copy.start()

    @pl.when(me == 0)
    def _():
        from_low[...] = jnp.zeros_like(from_low)

    @pl.when(me == count - 1)
    def _():
        from_high[...] = jnp.zeros_like(from_high)

    barrier = pltpu.get_barrier_semaphore()

    @pl.loop(0, 9)
    def _(i):
        for k in range(7):
            pl.semaphore_signal(
                barrier, inc=1, device_id=to_chan(lax.rem(me + 7 * i + k + 1, count)))

    lane_row = lax.broadcasted_iota(jnp.int32, (1, LANES), 1)
    channel = lax.rem(lane_row, CHANS)
    for ref in (g, y, part):
        ref[...] = jnp.zeros_like(ref)

    row = lax.broadcasted_iota(jnp.int32, (2 * LANES, 2 * LANES), 0)
    lane = lax.broadcasted_iota(jnp.int32, (2 * LANES, 2 * LANES), 1)
    mix[...] = jnp.where((row & 195) == (lane & 195), 1.0, 0.0).astype(BF16)
    rest = pl.ds(LANES * TILES, FLAT - LANES * TILES)
    for ref in (ct_re, ct_im, v_re, v_im):
        ref[rest, :] = jnp.zeros((FLAT - LANES * TILES, LANES), F32)

    for copy in small:
        copy.wait()
    for source, target in ((jones, g.at[0]), (duals, y)):
        turned = source[...].T
        for part_of, lanes in enumerate((slice(0, LANES), slice(LANES, 2 * LANES))):
            for half in range(2):
                size = min(HALF, STATIONS - HALF * half)
                target[pl.ds(SIDE * half + HALF * part_of, size), :] = (
                    turned[HALF * half:HALF * half + size, lanes])

    turned_rows = cbuf.reshape(FULL, 2 * LANES, LANES)
    place = (lane_row & 63) // CHANS
    vis_load.wait()

    def put(j, coherent, pairs):
        rows = pl.ds(LANES * j, LANES)
        turned = coherent.T
        values = [
            turned[:, :LANES].astype(F32),
            turned[:, LANES:].astype(F32),
            jnp.where(place == 2 * (j % GROUP), pairs, 0.0),
            jnp.where(place == 2 * (j % GROUP) + 1, pairs, 0.0),
        ]
        for ref, value in zip((ct_re, ct_im, v_re, v_im), values):
            if j == FULL:
                live = lax.broadcasted_iota(jnp.int32, (LANES, LANES), 0) < PAIRS - LANES * FULL
                value = jnp.where(live, value, 0.0)
            ref[rows, :] = value

    def put_group(first, size, load):
        load.wait()
        seen = [vbuf[:, LANES * j:LANES * (j + 1)] for j in range(first, first + size)]
        last = first + size == FULL
        if last:
            seen.append(jnp.concatenate(
                [vis_tail[:, 0, LANES:], jnp.zeros((16, 2 * LANES - vis_tail.shape[2]), F32)], axis=1))
        halves = []
        for pol in range(2):
            for each in seen:
                halves += [each[4 * pol:4 * pol + 4], each[8 + 4 * pol:12 + 4 * pol]]
            if len(seen) < GROUP:
                halves.append(jnp.zeros((8 * (GROUP - len(seen)), LANES), F32))
        pairs = jnp.concatenate(halves, axis=0).T
        for j in range(first, first + size):
            put(j, turned_rows[j], pairs)
        if last:
            put(FULL, jnp.concatenate(
                [coh_tail[:, :, LANES:], jnp.zeros((64, CHANS, 2 * LANES - coh_tail.shape[2]), BF16)],
                axis=2).reshape(2 * LANES, LANES), pairs)
        end = PAIRS if last else LANES * (first + size)
        for p in range(STATIONS):
            if LANES * first <= (STATIONS + 1) * p < end:
                for ref in (ct_re, ct_im):
                    ref[pl.ds((STATIONS + 1) * p, 1), :] = jnp.zeros((1, LANES), F32)

    def gain_row(p):
        return SIDE * (p // HALF) + p % HALF

    def model(p, gains):
        p_real = jnp.broadcast_to(gains[pl.ds(gain_row(p), 1), :], (STEP, LANES))
        p_imag = jnp.broadcast_to(gains[pl.ds(gain_row(p) + HALF, 1), :], (STEP, LANES))
        highs, lows = [], []
        for q in range(0, SIDE, STEP):
            pairs = pl.ds(nought + STATIONS * p + q, STEP)
            q_real = gains[pl.ds(gain_row(q), STEP), :]
            q_imag = gains[pl.ds(gain_row(q) + HALF, STEP), :]
            c_real = ct_re[pairs, :]
            c_imag = ct_im[pairs, :]
            half_real = c_real * q_real + c_imag * q_imag
            half_imag = c_imag * q_real - c_real * q_imag
            spot = pl.ds(SIDE * p + q, STEP)
            h_re[spot, :] = half_real
            h_im[spot, :] = half_imag
            m_real = (p_real * half_real - p_imag * half_imag) - v_re[pairs, :]
            m_imag = (p_real * half_imag + p_imag * half_real) - v_im[pairs, :]
            m = jnp.concatenate([m_real, m_imag], axis=1)
            high = m.astype(BF16)
            highs.append(high)
            lows.append((m - high.astype(F32)).astype(BF16))
        return highs, lows

    def gather_sums(p, sums):
        total = None
        for q in range(0, SIDE, 8):
            spot = pl.ds(SIDE * p + q, 8)
            a, b = h_re[spot, :], h_im[spot, :]
            u, w = sums[q:q + 8, :LANES], sums[q:q + 8, LANES:]
            three = (u * a + w * b, w * a - u * b, a * a + b * b)
            total = three if total is None else [x + y for x, y in zip(total, three)]
        for i in range(3):
            part[i, pl.ds(8 * p, 8), :] = total[i]

    def pass_over(first, end, gains):
        held = []
        for at in range(first, end, DOT):
            stations = range(at, min(at + DOT, end))
            models = [model(p, gains) for p in stations]
            lhs = jnp.concatenate(
                [x for side in (0, 1) for each in models for x in each[side]], axis=0)
            dot = jnp.dot(lhs, mix[...], preferred_element_type=F32)
            size = SIDE * len(stations)
            held.append((stations, dot[:size] + dot[size:]))
        for stations, total in held:
            for i, p in enumerate(stations):
                gather_sums(p, total[SIDE * i:SIDE * (i + 1)])

    def sums_of(half):
        out = []
        for i in range(3):
            tiles = []
            for t in range(4 * half, 4 * half + 4):
                total = part[i, pl.ds(64 * t, 8, stride=8), :]
                for s in range(1, 8):
                    total = total + part[i, pl.ds(64 * t + s, 8, stride=8), :]
                tiles.append(total)
            out.append(jnp.concatenate(tiles, axis=0))
        return jnp.concatenate(out[:2], axis=0), jnp.concatenate([out[2], out[2]], axis=0)

    def exchange(turn, half):
        rows = pl.ds(SIDE * half, SIDE)
        at = 2 * turn + half
        to_low = pltpu.make_async_remote_copy(
            sent.at[turn, rows], from_high.at[turn, rows], send_low.at[at], high_sem.at[at],
            device_id=to_chan(me - 1))
        to_high = pltpu.make_async_remote_copy(
            sent.at[turn, rows], from_low.at[turn, rows], send_high.at[at], low_sem.at[at],
            device_id=to_chan(me + 1))
        return to_low, to_high

    def send(turn, half):
        to_low, to_high = exchange(turn, half)

        @pl.when(me > 0)
        def _():
            to_low.start()

        @pl.when(me < count - 1)
        def _():
            to_high.start()

    def receive(turn, half):
        to_low, to_high = exchange(turn, half)

        @pl.when(me > 0)
        def _():
            to_low.wait_send()
            to_high.wait_recv()

        @pl.when(me < count - 1)
        def _():
            to_high.wait_send()
            to_low.wait_recv()

    def column_sums(x):
        return jnp.sum(x, axis=0, keepdims=True)

    def residuals(gap, moved, before):
        now = [column_sums(gap * gap), column_sums(moved * moved) * (penalty * penalty)]
        return now if before is None else [x + y for x, y in zip(before, now)]

    def rows_of(half):
        return pl.ds(SIDE * half, SIDE)

    def first_update(half):
        rows = rows_of(half)
        numer, denom = sums_of(half)
        gain0 = g[0, rows, :]
        dual0 = y[rows, :]
        gain1 = (gain0 * denom - numer + penalty * (gain0 - dual0)) / (denom + penalty)
        summed = gain1 + dual0
        g[1, rows, :] = gain1
        sent[0, rows, :] = summed
        if half == 0:
            pl.semaphore_wait(barrier, count - 1)
        send(0, half)
        kept[0, rows, :] = smooth_own(summed, channel)

    for half in range(2):
        for load in loads[2 * half:2 * half + 2]:
            put_group(*load)
        pass_over(HALF * half, min(HALF * half + HALF, STATIONS), g.at[0])
        first_update(half)

    first = None
    for half in range(2):
        rows = rows_of(half)
        pass_over(HALF * half, min(HALF * half + HALF, STATIONS), g.at[1])
        numer, denom = sums_of(half)
        receive(0, half)
        gain1 = g[1, rows, :]
        fresh1 = kept[0, rows, :] + smooth_sides(
            from_low[0, rows, :], from_high[0, rows, :], channel)
        dual1 = y[rows, :] + gain1 - fresh1
        gain2 = (gain1 * denom - numer + penalty * (fresh1 - dual1)) / (denom + penalty)
        summed = gain2 + dual1
        sent[1, rows, :] = summed
        send(1, half)
        first = residuals(gain1 - fresh1, fresh1 - g[0, rows, :], first)
        kept[1, rows, :] = smooth_own(summed, channel)
        kept[2, rows, :] = gain2
        kept[3, rows, :] = fresh1
        kept[4, rows, :] = dual1

    outs = []

    def turned_out(x, ref):
        both = jnp.concatenate(
            [jnp.concatenate([x[:HALF], x[SIDE:SIDE + HALF]], axis=0),
             jnp.concatenate([x[HALF:SIDE], x[SIDE + HALF:]], axis=0)], axis=1).T
        at = len(outs)
        gains_buf[at] = both[:, :STATIONS]
        outs.append(pltpu.make_async_copy(gains_buf.at[at], ref, out_sems.at[at]))
        outs[-1].start()

    turned_out(kept[2], jones_out)
    second = None
    for half in range(2):
        rows = rows_of(half)
        receive(1, half)
        fresh2 = kept[1, rows, :] + smooth_sides(
            from_low[1, rows, :], from_high[1, rows, :], channel)
        gap = kept[2, rows, :] - fresh2
        second = residuals(gap, fresh2 - kept[3, rows, :], second)
        kept[0, rows, :] = fresh2
        kept[4, rows, :] = kept[4, rows, :] + gap
    four = jnp.sum(jnp.concatenate(first + second, axis=0), axis=1, keepdims=True)
    own_lane = lax.broadcasted_iota(jnp.int32, (4, LANES), 0) == lax.broadcasted_iota(
        jnp.int32, (4, LANES), 1)
    mine[...] = jnp.sum(jnp.where(own_lane, four, 0.0), axis=0, keepdims=True)

    rank = lax.rem(me // 2, 8) * 8 + me // 16 * 2 + lax.rem(me, 2)

    @pl.loop(0, 9)
    def _(i):
        for k in range(7):
            other = 7 * i + k
            other = other + (other >= rank).astype(jnp.int32)
            peer = lax.rem(other, 8) // 2 * 16 + other // 8 * 2 + lax.rem(other, 2)
            pltpu.make_async_remote_copy(
                mine, gathered.at[me], norm_send, norm_recv, device_id=to_chan(peer)).start()

    gathered[me] = mine[...]
    turned_out(kept[0], cons_out)
    turned_out(kept[4], duals_out)
    others = gathered.at[pl.ds(0, count - 1)]
    pltpu.make_async_copy(others, others, norm_recv).wait()
    pltpu.make_async_copy(others, others, norm_send).wait()
    total = jnp.sum(gathered[...], axis=0) / entries
    norms_buf[...] = jnp.concatenate(
        [total[:, :2], pltpu.roll(total, LANES - 2, axis=1)[:, :2]], axis=0)
    outs.append(pltpu.make_async_copy(norms_buf, norms_out, out_sems.at[3]))
    outs[-1].start()
    for copy in outs:
        copy.wait()


def write_out(*refs):
    sems = refs[-1]
    into = [pltpu.make_async_copy(refs[i], refs[8 + i], sems.at[i]) for i in range(4)]
    onward = [pltpu.make_async_copy(refs[8 + i], refs[4 + i], sems.at[i]) for i in range(4)]
    for copy in into:
        copy.start()
    for first, second in zip(into, onward):
        first.wait()
        second.start()
    for copy in onward:
        copy.wait()


def local(visibility, coherency, jones_start, duals_start):
    shape = jones_start.shape
    entries = jones_start.size * lax.axis_size("chan")
    vis = visibility.reshape(16, 1, PAIRS)
    coh = coherency.reshape(64, CHANS, PAIRS)
    jones = jones_start.reshape(256, STATIONS)
    duals = duals_start.reshape(256, STATIONS)
    hbm = pl.BlockSpec(memory_space=pltpu.HBM)
    gains = jax.ShapeDtypeStruct((256, STATIONS), F32)
    pairs = pltpu.VMEM((FLAT, LANES), F32)
    grid_pairs = pltpu.VMEM((SIDE * SIDE, LANES), F32)
    dma = pltpu.SemaphoreType.DMA
    out = pl.pallas_call(
        functools.partial(body, entries=entries),
        out_shape=[gains, gains, gains, jax.ShapeDtypeStruct((2, 2), F32)],
        in_specs=[hbm] * 4,
        out_specs=[hbm] * 4,
        scratch_shapes=[
            pltpu.VMEM((3, 256, STATIONS), F32),
            pltpu.VMEM((2, 2), F32),
            dma((4,)),
            pltpu.VMEM((256, STATIONS), F32),
            pltpu.VMEM((256, STATIONS), F32),
            pltpu.VMEM((16, 1, PAIRS - LANES * (FULL - 1)), F32),
            pltpu.VMEM((64, CHANS, PAIRS - LANES * (FULL - 1)), BF16),
            dma((4,)),
            pltpu.VMEM((FULL, 64, CHANS, LANES), BF16),
            pltpu.VMEM((16, LANES * FULL), F32),
            pairs, pairs, pairs, pairs,
            grid_pairs, grid_pairs,
            pltpu.VMEM((2 * LANES, 2 * LANES), BF16),
            pltpu.VMEM((2, 2 * SIDE, LANES), F32),
            pltpu.VMEM((2 * SIDE, LANES), F32),
            pltpu.VMEM((3, 8 * SIDE, LANES), F32),
            pltpu.VMEM((5, 2 * SIDE, LANES), F32),
            pltpu.VMEM((2, 2 * SIDE, LANES), F32),
            pltpu.VMEM((2, 2 * SIDE, LANES), F32),
            pltpu.VMEM((2, 2 * SIDE, LANES), F32),
            pltpu.VMEM((1, LANES), F32),
            pltpu.VMEM((lax.axis_size("chan"), 1, LANES), F32),
            dma((-(-FULL // GROUP),)), dma, dma((4,)), dma((4,)), dma((4,)), dma((4,)),
            dma, dma,
        ],
        compiler_params=pltpu.CompilerParams(
            vmem_limit_bytes=VMEM_LIMIT, collective_id=0, has_side_effects=True),
    )(vis, coh, jones, duals)
    anywhere = pl.BlockSpec(memory_space=pl.ANY)
    out = pl.pallas_call(
        write_out,
        out_shape=[jax.ShapeDtypeStruct(part.shape, part.dtype) for part in out],
        in_specs=[anywhere] * 4,
        out_specs=[anywhere] * 4,
        scratch_shapes=[pltpu.VMEM(part.shape, part.dtype) for part in out] + [dma((4,))],
    )(*out)
    return tuple(part.reshape(shape) for part in out[:3]) + (out[3],)


def solution(mesh):
    gain = P(None, None, "slot", "chan", None)
    return jax.shard_map(
        local,
        mesh=mesh,
        in_specs=(P(None, None, "chan", "slot", None), P(None, None, None, "chan", "slot", None), gain, gain),
        out_specs=(gain, gain, gain, P("slot", None)),
        check_vma=False,
    )
```

```python
import functools

import jax
import jax.numpy as jnp
from jax import lax
from jax.experimental import pallas as pl
from jax.experimental.pallas import tpu as pltpu
from jax.sharding import PartitionSpec as P

STATIONS = 62
SIDE = 64
CHANS = 4
PAIRS = STATIONS * STATIONS
LANES = 128
FULL = PAIRS // LANES
TILES = FULL + 1
FLAT = STATIONS * SIDE + 2 * SIDE
HALF = SIDE // 2
GROUP = 8
DOT = 2
STEP = 16
VMEM_LIMIT = 65_500_000

penalty = 8.0
kernel_taps = (0.04, 0.06, 0.1, 0.15, 0.3, 0.15, 0.1, 0.06, 0.04)
F32 = jnp.float32
BF16 = jnp.bfloat16


def to_chan(index):
    return {"chan": index}


def shifted(x, by):
    return x if by == 0 else pltpu.roll(x, (-by) % LANES, axis=1)


def smooth_own(own, channel):
    total = None
    for o in range(-3, 4):
        weight = jnp.where((channel + o >= 0) & (channel + o < CHANS), kernel_taps[o + 4], 0.0)
        term = shifted(own, o) * weight
        total = term if total is None else total + term
    return total


def smooth_sides(low, high, channel):
    total = None
    for o in range(1, 5):
        weight = jnp.where(channel - o < 0, kernel_taps[4 - o], 0.0)
        term = shifted(low, CHANS - o) * weight
        total = term if total is None else total + term
        weight = jnp.where(channel + o >= CHANS, kernel_taps[4 + o], 0.0)
        total = total + shifted(high, o - CHANS) * weight
    return total


def body(
    vis, coh, jones_in, duals_in,
    jones_out, cons_out, duals_out, norms_out,
    gains_buf, norms_buf, out_sems,
    jones, duals, vis_tail, coh_tail, in_sems,
    cbuf, vbuf, ct_re, ct_im, v_re, v_im, h_re, h_im, mix,
    g, y, part, kept, sent, from_low, from_high, mine, gathered,
    load_sems, vis_sem, send_low, send_high, low_sem, high_sem,
    norm_send, norm_recv,
    *, entries,
):
    count = lax.axis_size("chan")
    me = lax.axis_index("chan")
    nought = lax.div(me, 1024)
    loads = []
    for first in range(0, FULL, GROUP):
        size = min(GROUP, FULL - first)
        sem = load_sems.at[first // GROUP]
        for j in range(first, first + size):
            pltpu.make_async_copy(
                coh.at[:, :, pl.ds(LANES * j, LANES)], cbuf.at[j], sem).start()
        span = cbuf.at[pl.ds(first, size)]
        loads.append((first, size, pltpu.make_async_copy(span, span, sem)))
        if first == 0:
            vis_load = pltpu.make_async_copy(
                vis.at[:, 0, pl.ds(0, LANES * FULL)], vbuf, vis_sem)
            vis_load.start()
            ends = pl.ds(LANES * (FULL - 1), PAIRS - LANES * (FULL - 1))
            small = [
                pltpu.make_async_copy(jones_in, jones, in_sems.at[0]),
                pltpu.make_async_copy(duals_in, duals, in_sems.at[1]),
                pltpu.make_async_copy(vis.at[:, :, ends], vis_tail, in_sems.at[2]),
                pltpu.make_async_copy(coh.at[:, :, ends], coh_tail, in_sems.at[3]),
            ]
            for copy in small:
                copy.start()

    @pl.when(me == 0)
    def _():
        from_low[...] = jnp.zeros_like(from_low)

    @pl.when(me == count - 1)
    def _():
        from_high[...] = jnp.zeros_like(from_high)

    barrier = pltpu.get_barrier_semaphore()

    @pl.loop(0, 9)
    def _(i):
        for k in range(7):
            pl.semaphore_signal(
                barrier, inc=1, device_id=to_chan(lax.rem(me + 7 * i + k + 1, count)))

    lane_row = lax.broadcasted_iota(jnp.int32, (1, LANES), 1)
    channel = lax.rem(lane_row, CHANS)
    for ref in (g, y, part):
        ref[...] = jnp.zeros_like(ref)

    row = lax.broadcasted_iota(jnp.int32, (2 * LANES, 2 * LANES), 0)
    lane = lax.broadcasted_iota(jnp.int32, (2 * LANES, 2 * LANES), 1)
    mix[...] = jnp.where((row & 195) == (lane & 195), 1.0, 0.0).astype(BF16)
    rest = pl.ds(LANES * TILES, FLAT - LANES * TILES)
    for ref in (ct_re, ct_im, v_re, v_im):
        ref[rest, :] = jnp.zeros((FLAT - LANES * TILES, LANES), F32)

    for copy in small:
        copy.wait()
    for source, target in ((jones, g.at[0]), (duals, y)):
        turned = source[...].T
        for part_of, lanes in enumerate((slice(0, LANES), slice(LANES, 2 * LANES))):
            for half in range(2):
                size = min(HALF, STATIONS - HALF * half)
                target[pl.ds(SIDE * half + HALF * part_of, size), :] = (
                    turned[HALF * half:HALF * half + size, lanes])

    turned_rows = cbuf.reshape(FULL, 2 * LANES, LANES)
    place = (lane_row & 63) // CHANS
    vis_load.wait()

    def put(j, coherent, pairs):
        rows = pl.ds(LANES * j, LANES)
        turned = coherent.T
        values = [
            turned[:, :LANES].astype(F32),
            turned[:, LANES:].astype(F32),
            jnp.where(place == 2 * (j % GROUP), pairs, 0.0),
            jnp.where(place == 2 * (j % GROUP) + 1, pairs, 0.0),
        ]
        for ref, value in zip((ct_re, ct_im, v_re, v_im), values):
            if j == FULL:
                live = lax.broadcasted_iota(jnp.int32, (LANES, LANES), 0) < PAIRS - LANES * FULL
                value = jnp.where(live, value, 0.0)
            ref[rows, :] = value

    def put_group(first, size, load):
        load.wait()
        seen = [vbuf[:, LANES * j:LANES * (j + 1)] for j in range(first, first + size)]
        last = first + size == FULL
        if last:
            seen.append(jnp.concatenate(
                [vis_tail[:, 0, LANES:], jnp.zeros((16, 2 * LANES - vis_tail.shape[2]), F32)], axis=1))
        halves = []
        for pol in range(2):
            for each in seen:
                halves += [each[4 * pol:4 * pol + 4], each[8 + 4 * pol:12 + 4 * pol]]
            if len(seen) < GROUP:
                halves.append(jnp.zeros((8 * (GROUP - len(seen)), LANES), F32))
        pairs = jnp.concatenate(halves, axis=0).T
        for j in range(first, first + size):
            put(j, turned_rows[j], pairs)
        if last:
            put(FULL, jnp.concatenate(
                [coh_tail[:, :, LANES:], jnp.zeros((64, CHANS, 2 * LANES - coh_tail.shape[2]), BF16)],
                axis=2).reshape(2 * LANES, LANES), pairs)
        end = PAIRS if last else LANES * (first + size)
        for p in range(STATIONS):
            if LANES * first <= (STATIONS + 1) * p < end:
                for ref in (ct_re, ct_im):
                    ref[pl.ds((STATIONS + 1) * p, 1), :] = jnp.zeros((1, LANES), F32)

    def gain_row(p):
        return SIDE * (p // HALF) + p % HALF

    def model(p, gains):
        p_real = jnp.broadcast_to(gains[pl.ds(gain_row(p), 1), :], (STEP, LANES))
        p_imag = jnp.broadcast_to(gains[pl.ds(gain_row(p) + HALF, 1), :], (STEP, LANES))
        highs, lows = [], []
        for q in range(0, SIDE, STEP):
            pairs = pl.ds(nought + STATIONS * p + q, STEP)
            q_real = gains[pl.ds(gain_row(q), STEP), :]
            q_imag = gains[pl.ds(gain_row(q) + HALF, STEP), :]
            c_real = ct_re[pairs, :]
            c_imag = ct_im[pairs, :]
            half_real = c_real * q_real + c_imag * q_imag
            half_imag = c_imag * q_real - c_real * q_imag
            spot = pl.ds(SIDE * p + q, STEP)
            h_re[spot, :] = half_real
            h_im[spot, :] = half_imag
            m_real = (p_real * half_real - p_imag * half_imag) - v_re[pairs, :]
            m_imag = (p_real * half_imag + p_imag * half_real) - v_im[pairs, :]
            m = jnp.concatenate([m_real, m_imag], axis=1)
            high = m.astype(BF16)
            highs.append(high)
            lows.append((m - high.astype(F32)).astype(BF16))
        return highs, lows

    def gather_sums(p, sums):
        total = None
        for q in range(0, SIDE, 8):
            spot = pl.ds(SIDE * p + q, 8)
            a, b = h_re[spot, :], h_im[spot, :]
            u, w = sums[q:q + 8, :LANES], sums[q:q + 8, LANES:]
            three = (u * a + w * b, w * a - u * b, a * a + b * b)
            total = three if total is None else [x + y for x, y in zip(total, three)]
        for i in range(3):
            part[i, pl.ds(8 * p, 8), :] = total[i]

    def pass_over(first, end, gains):
        held = []
        for at in range(first, end, DOT):
            stations = range(at, min(at + DOT, end))
            models = [model(p, gains) for p in stations]
            lhs = jnp.concatenate(
                [x for side in (0, 1) for each in models for x in each[side]], axis=0)
            dot = jnp.dot(lhs, mix[...], preferred_element_type=F32)
            size = SIDE * len(stations)
            held.append((stations, dot[:size] + dot[size:]))
        for stations, total in held:
            for i, p in enumerate(stations):
                gather_sums(p, total[SIDE * i:SIDE * (i + 1)])

    def sums_of(half):
        out = []
        for i in range(3):
            tiles = []
            for t in range(4 * half, 4 * half + 4):
                total = part[i, pl.ds(64 * t, 8, stride=8), :]
                for s in range(1, 8):
                    total = total + part[i, pl.ds(64 * t + s, 8, stride=8), :]
                tiles.append(total)
            out.append(jnp.concatenate(tiles, axis=0))
        return jnp.concatenate(out[:2], axis=0), jnp.concatenate([out[2], out[2]], axis=0)

    def exchange(turn, half):
        rows = pl.ds(SIDE * half, SIDE)
        at = 2 * turn + half
        to_low = pltpu.make_async_remote_copy(
            sent.at[turn, rows], from_high.at[turn, rows], send_low.at[at], high_sem.at[at],
            device_id=to_chan(me - 1))
        to_high = pltpu.make_async_remote_copy(
            sent.at[turn, rows], from_low.at[turn, rows], send_high.at[at], low_sem.at[at],
            device_id=to_chan(me + 1))
        return to_low, to_high

    def send(turn, half):
        to_low, to_high = exchange(turn, half)

        @pl.when(me > 0)
        def _():
            to_low.start()

        @pl.when(me < count - 1)
        def _():
            to_high.start()

    def receive(turn, half):
        to_low, to_high = exchange(turn, half)

        @pl.when(me > 0)
        def _():
            to_low.wait_send()
            to_high.wait_recv()

        @pl.when(me < count - 1)
        def _():
            to_high.wait_send()
            to_low.wait_recv()

    def column_sums(x):
        return jnp.sum(x, axis=0, keepdims=True)

    def residuals(gap, moved, before):
        now = [column_sums(gap * gap), column_sums(moved * moved) * (penalty * penalty)]
        return now if before is None else [x + y for x, y in zip(before, now)]

    def rows_of(half):
        return pl.ds(SIDE * half, SIDE)

    def first_update(half):
        rows = rows_of(half)
        numer, denom = sums_of(half)
        gain0 = g[0, rows, :]
        dual0 = y[rows, :]
        gain1 = (gain0 * denom - numer + penalty * (gain0 - dual0)) / (denom + penalty)
        summed = gain1 + dual0
        g[1, rows, :] = gain1
        sent[0, rows, :] = summed
        if half == 0:
            pl.semaphore_wait(barrier, count - 1)
        send(0, half)
        kept[0, rows, :] = smooth_own(summed, channel)

    for half in range(2):
        for load in loads[2 * half:2 * half + 2]:
            put_group(*load)
        pass_over(HALF * half, min(HALF * half + HALF, STATIONS), g.at[0])
        first_update(half)

    first = None
    for half in range(2):
        rows = rows_of(half)
        pass_over(HALF * half, min(HALF * half + HALF, STATIONS), g.at[1])
        numer, denom = sums_of(half)
        receive(0, half)
        gain1 = g[1, rows, :]
        fresh1 = kept[0, rows, :] + smooth_sides(
            from_low[0, rows, :], from_high[0, rows, :], channel)
        dual1 = y[rows, :] + gain1 - fresh1
        gain2 = (gain1 * denom - numer + penalty * (fresh1 - dual1)) / (denom + penalty)
        summed = gain2 + dual1
        sent[1, rows, :] = summed
        send(1, half)
        first = residuals(gain1 - fresh1, fresh1 - g[0, rows, :], first)
        kept[1, rows, :] = smooth_own(summed, channel)
        kept[2, rows, :] = gain2
        kept[3, rows, :] = fresh1
        kept[4, rows, :] = dual1

    outs = []

    def turned_out(x, ref):
        both = jnp.concatenate(
            [jnp.concatenate([x[:HALF], x[SIDE:SIDE + HALF]], axis=0),
             jnp.concatenate([x[HALF:SIDE], x[SIDE + HALF:]], axis=0)], axis=1).T
        at = len(outs)
        gains_buf[at] = both[:, :STATIONS]
        outs.append(pltpu.make_async_copy(gains_buf.at[at], ref, out_sems.at[at]))
        outs[-1].start()

    turned_out(kept[2], jones_out)
    second = None
    for half in range(2):
        rows = rows_of(half)
        receive(1, half)
        fresh2 = kept[1, rows, :] + smooth_sides(
            from_low[1, rows, :], from_high[1, rows, :], channel)
        gap = kept[2, rows, :] - fresh2
        second = residuals(gap, fresh2 - kept[3, rows, :], second)
        kept[0, rows, :] = fresh2
        kept[4, rows, :] = kept[4, rows, :] + gap
    four = jnp.sum(jnp.concatenate(first + second, axis=0), axis=1, keepdims=True)
    mine[...] = jnp.where(
        lane_row == 0,
        jnp.concatenate([four[0:1], four[2:3]], axis=0),
        jnp.concatenate([four[1:2], four[3:4]], axis=0))

    rank = lax.rem(me // 2, 8) * 8 + me // 16 * 2 + lax.rem(me, 2)

    @pl.loop(0, 9)
    def _(i):
        for k in range(7):
            other = 7 * i + k
            other = other + (other >= rank).astype(jnp.int32)
            peer = lax.rem(other, 8) // 2 * 16 + other // 8 * 2 + lax.rem(other, 2)
            pltpu.make_async_remote_copy(
                mine, gathered.at[me], norm_send, norm_recv, device_id=to_chan(peer)).start()

    gathered[me] = mine[...]
    turned_out(kept[0], cons_out)
    turned_out(kept[4], duals_out)
    others = gathered.at[pl.ds(0, count - 1)]
    pltpu.make_async_copy(others, others, norm_recv).wait()
    total = jnp.sum(gathered[...], axis=0) / entries
    norms_buf[...] = total[:, :2]
    outs.append(pltpu.make_async_copy(norms_buf, norms_out, out_sems.at[3]))
    outs[-1].start()
    pltpu.make_async_copy(others, others, norm_send).wait()
    for copy in outs:
        copy.wait()


def write_out(*refs):
    sems = refs[-1]
    into = [pltpu.make_async_copy(refs[i], refs[8 + i], sems.at[i]) for i in range(4)]
    onward = [pltpu.make_async_copy(refs[8 + i], refs[4 + i], sems.at[i]) for i in range(4)]
    for copy in into:
        copy.start()
    for first, second in zip(into, onward):
        first.wait()
        second.start()
    for copy in onward:
        copy.wait()


def local(visibility, coherency, jones_start, duals_start):
    shape = jones_start.shape
    entries = jones_start.size * lax.axis_size("chan")
    vis = visibility.reshape(16, 1, PAIRS)
    coh = coherency.reshape(64, CHANS, PAIRS)
    jones = jones_start.reshape(256, STATIONS)
    duals = duals_start.reshape(256, STATIONS)
    hbm = pl.BlockSpec(memory_space=pltpu.HBM)
    gains = jax.ShapeDtypeStruct((256, STATIONS), F32)
    pairs = pltpu.VMEM((FLAT, LANES), F32)
    grid_pairs = pltpu.VMEM((SIDE * SIDE, LANES), F32)
    dma = pltpu.SemaphoreType.DMA
    out = pl.pallas_call(
        functools.partial(body, entries=entries),
        out_shape=[gains, gains, gains, jax.ShapeDtypeStruct((2, 2), F32)],
        in_specs=[hbm] * 4,
        out_specs=[hbm] * 4,
        scratch_shapes=[
            pltpu.VMEM((3, 256, STATIONS), F32),
            pltpu.VMEM((2, 2), F32),
            dma((4,)),
            pltpu.VMEM((256, STATIONS), F32),
            pltpu.VMEM((256, STATIONS), F32),
            pltpu.VMEM((16, 1, PAIRS - LANES * (FULL - 1)), F32),
            pltpu.VMEM((64, CHANS, PAIRS - LANES * (FULL - 1)), BF16),
            dma((4,)),
            pltpu.VMEM((FULL, 64, CHANS, LANES), BF16),
            pltpu.VMEM((16, LANES * FULL), F32),
            pairs, pairs, pairs, pairs,
            grid_pairs, grid_pairs,
            pltpu.VMEM((2 * LANES, 2 * LANES), BF16),
            pltpu.VMEM((2, 2 * SIDE, LANES), F32),
            pltpu.VMEM((2 * SIDE, LANES), F32),
            pltpu.VMEM((3, 8 * SIDE, LANES), F32),
            pltpu.VMEM((5, 2 * SIDE, LANES), F32),
            pltpu.VMEM((2, 2 * SIDE, LANES), F32),
            pltpu.VMEM((2, 2 * SIDE, LANES), F32),
            pltpu.VMEM((2, 2 * SIDE, LANES), F32),
            pltpu.VMEM((2, LANES), F32),
            pltpu.VMEM((lax.axis_size("chan"), 2, LANES), F32),
            dma((-(-FULL // GROUP),)), dma, dma((4,)), dma((4,)), dma((4,)), dma((4,)),
            dma, dma,
        ],
        compiler_params=pltpu.CompilerParams(
            vmem_limit_bytes=VMEM_LIMIT, collective_id=0, has_side_effects=True),
    )(vis, coh, jones, duals)
    anywhere = pl.BlockSpec(memory_space=pl.ANY)
    out = pl.pallas_call(
        write_out,
        out_shape=[jax.ShapeDtypeStruct(part.shape, part.dtype) for part in out],
        in_specs=[anywhere] * 4,
        out_specs=[anywhere] * 4,
        scratch_shapes=[pltpu.VMEM(part.shape, part.dtype) for part in out] + [dma((4,))],
    )(*out)
    return tuple(part.reshape(shape) for part in out[:3]) + (out[3],)


def solution(mesh):
    gain = P(None, None, "slot", "chan", None)
    return jax.shard_map(
        local,
        mesh=mesh,
        in_specs=(P(None, None, "chan", "slot", None), P(None, None, None, "chan", "slot", None), gain, gain),
        out_specs=(gain, gain, gain, P("slot", None)),
        check_vma=False,
    )
```
